32 devices in a mesh: subj: 4 (over y, core), vox: 8 (over z, x).
Axes of the slice: x: 2, y: 2, z: 4, core: 2. Of those that a mesh axis runs over, the one named last changes fastest.
Arguments:
- series: bfloat16 [16, 256, 16384], P('subj', None, 'vox'), may hold values from -6 to 6
- offsets: int32 [16, 12], replicated, may hold values from 0 to 240
- selected: int32 [16], replicated, may hold values from 0 to 16383, as said below
Outputs:
- kernel: float32 [16, 192, 192], P('vox', 'subj')
The draws below stay inside these ranges and needn't reach their ends.
Inputs may be any that keep to these rules, and one draw needn't show every extreme that they name: `offsets`: each epoch lies inside its subject's run; epochs may intersect. `selected`: the ids are distinct.
All inputs are finite; a program needn't handle non-finite values.
Results may differ from the reference program's by a relative error of at most 0.00035.
Values may be sent and summed in bfloat16 or wider, within the bound.
A program may use at most 128 MiB of HBM per device.

```python
import jax
import jax.numpy as jnp
from jax import lax

VOX = 16384
TR = 16
EP = 12
RUN_TR = 256
SUBJECTS = 16
SEL = 16


def draw_selected(key, part):
    first_key = jax.random.fold_in(key, 11)
    second_key = jax.random.fold_in(key, 12)
    middle = jax.random.permutation(first_key, VOX - 2)[:SEL - 2] + 1
    ends = jnp.array([0, VOX - 1], dtype=jnp.int32)
    joined = jnp.concatenate([ends, middle.astype(jnp.int32)])
    return jax.random.permutation(second_key, joined).astype(jnp.int32)


def plant(entries, stream_key, least, high):
    extent = entries.shape
    place = [jax.random.randint(jax.random.fold_in(stream_key, axis), (), 0, extent[axis]) for axis in range(len(extent))]
    entries = entries.at[tuple(place)].set(least)
    longest = extent.index(max(extent))
    place[longest] = (place[longest] + 1) % extent[longest]
    return entries.at[tuple(place)].set(high)


def block_levels(key, shape, cuts, smallest, top_value):
    def one(position, parts):
        steps = jax.random.uniform(jax.random.fold_in(jax.random.fold_in(key, 6), position), (parts,), jnp.float32, smallest / len(cuts), top_value / len(cuts))
        return jnp.repeat(jnp.exp(steps), shape[position] // parts).reshape((-1,) + (1,) * (len(shape) - position - 1))

    gain = one(*cuts[0])
    for cut in cuts[1:]:
        gain = gain * one(*cut)
    return gain


def bell_draw(key, dims, scale, reach, cuts=(), held_as=jnp.bfloat16):
    entries = scale * jax.random.normal(key, dims, jnp.float32)
    if cuts:
        entries = entries * block_levels(key, dims, cuts, -0.22, 0.18)
    return jnp.clip(entries, -reach, reach).astype(held_as)


def setup_inputs(seed: int = 0) -> dict:
    keys = jax.random.split(jax.random.key(seed), 4)
    return {
        "series": bell_draw(keys[0], (SUBJECTS, RUN_TR, VOX), 1.0, 6.0, ((0, 4), (2, 8))),
        "offsets": plant(jax.random.randint(keys[1], (SUBJECTS, EP), 0, RUN_TR - TR + 1), jax.random.fold_in(keys[1], 1), 0, RUN_TR - TR).astype(jnp.int32),
        "selected": draw_selected(jax.random.fold_in(keys[3], 71), 0),
    }


series_floor = 1.0
spread_floor = 0.05
shrink_factor = 0.9

def windows(block, starts):

    def subject_windows(subject_row, subject_offsets):
        return jax.vmap(lambda offset: lax.dynamic_slice_in_dim(subject_row, offset, TR, 0))(subject_offsets)
    return jax.vmap(subject_windows)(block, starts)

def standardize(values):
    centred = values - lax.optimization_barrier(jnp.mean(values, axis=2, keepdims=True))
    return centred / jnp.sqrt(lax.optimization_barrier(jnp.sum(centred * centred, axis=2, keepdims=True)) + series_floor)

def fisher_transform(correlation):
    shrunk = shrink_factor * correlation
    return 0.5 * jnp.log((1.0 + shrunk) / (1.0 - shrunk))

def scores(slab_std, voxel_std):
    correlation = jnp.einsum('setk,setv->ksev', slab_std, voxel_std, precision=lax.Precision.HIGHEST)
    fisher = fisher_transform(correlation)
    centred = fisher - lax.optimization_barrier(jnp.mean(fisher, axis=2, keepdims=True))
    variance = lax.optimization_barrier(jnp.mean(centred * centred, axis=2, keepdims=True))
    zscored = (centred / jnp.sqrt(variance + spread_floor)).astype(jnp.bfloat16)
    return zscored.reshape(zscored.shape[0], zscored.shape[1] * zscored.shape[2], zscored.shape[3])

def reference(series, offsets, selected):
    epochs = windows(series, offsets)
    voxel_std = standardize(epochs.astype(jnp.float32))
    slab_std = standardize(jnp.take(epochs, selected, axis=3).astype(jnp.float32))
    block_width = 8
    blocks = jnp.moveaxis(slab_std.reshape(slab_std.shape[:3] + (SEL // block_width, block_width)), 3, 0)

    def kernel_block(slab_block):
        zscored = scores(slab_block, voxel_std).astype(jnp.float32)
        return jnp.einsum('kev,kfv->kef', zscored, zscored, precision=lax.Precision.HIGHEST) * (1.0 / VOX)
    mapped = lax.map(kernel_block, blocks)
    return mapped.reshape(SEL, mapped.shape[2], mapped.shape[3])
```

```python
import functools

import jax
import jax.numpy as jnp
from jax import lax
from jax.experimental import pallas as pl
from jax.experimental.pallas import tpu as pltpu
from jax.sharding import PartitionSpec as P

TR = 16
KB = 8
C1 = 4
series_floor = 1.0
spread_floor = 0.05
shrink_factor = 0.9
f32 = jnp.float32
bf16 = jnp.bfloat16


def iota(shape, dim):
    return lax.broadcasted_iota(jnp.int32, shape, dim)


def up8(n):
    return -(-n // 8) * 8


def pieces_of(G, V, NE):
    R = V
    while R > G and (V % R or R % G or (G * NE) % R or (G * NE // R) % 8):
        R -= 1
    return R


def kernel(
    G, V, NS, EP, SEL, W,
    off_ref, sel_ref, series_hbm, out_ref,
    series_ref, load_sem, ep, hot, inv, part, slots, a_hi, a_lo, perm, send, recv,
    expand, gram, pieces_in, summed, landed, direct,
    slab_send, slab_recv, sc_send, sc_recv, last_send, last_recv,
    rs_send, rs_recv, fin_send, fin_recv, dir_send, dir_recv,
):
    subj = lax.axis_index("subj")
    vox = lax.axis_index("vox")
    RUN = series_ref.shape[1]
    VL = series_ref.shape[2]
    ROWS = EP * TR
    H = SEL // KB
    KH = KB // G
    SL = SEL // V
    NE = NS * EP
    chunks = VL // W
    R = pieces_of(G, V, NE)
    VR = V // R
    RP = G * NE // R
    PG = R // G
    T = H * KH
    E1 = EP - 1
    NR = NS * E1
    BR = send.shape[2]
    starts = tuple(i * NR // 8 * 8 for i in range(KH))
    HG = G // 2
    shift = V // 2 + G // 2
    half = subj // HG
    cross = [(1 - half) * HG + b for b in range(HG)]
    near = [half * HG + lax.rem(subj + d, HG) for d in range(1, HG)]
    Q = last_recv.shape[0] - 1
    QC = VL // Q

    barrier = pltpu.get_barrier_semaphore()
    for d in range(1, G):
        pl.semaphore_signal(
            barrier, inc=1, device_id=(lax.rem(subj + d, G), vox),
            device_id_type=pl.DeviceIdType.MESH,
        )
    for d in range(1, V):
        pl.semaphore_signal(
            barrier, inc=1, device_id=(subj, lax.rem(vox + d, V)),
            device_id_type=pl.DeviceIdType.MESH,
        )

    def load(s):
        return pltpu.make_async_copy(series_hbm.at[s], series_ref.at[s], load_sem.at[s])

    for s in range(NS):
        load(s).start()

    ids = jnp.zeros((SEL, 1), jnp.int32)
    which = iota((SEL, 1), 0)
    for p in range(SEL):
        ids = jnp.where(which == p, sel_ref[(p + shift) % V * SL + p // V], ids)
    picker = jnp.where(iota((SEL, VL), 1) + vox * VL == ids, 1.0, 0.0).astype(bf16)
    col = iota((TR, RUN), 1) - iota((TR, RUN), 0)
    pieces = []
    for s in range(NS):
        tiles = [
            jnp.where(col == off_ref[subj * NS + s, e], 1.0, 0.0) for e in range(EP)
        ]
        hot[s] = jnp.concatenate(tiles, axis=0).astype(bf16)
    for s in range(NS):
        load(s).wait()
        runs = lax.dot_general(
            picker, series_ref[s], (((1,), (1,)), ((), ())), preferred_element_type=f32
        )
        pieces.append(lax.dot_general(
            runs.astype(bf16), hot[s], (((1,), (1,)), ((), ())), preferred_element_type=f32
        ))
    joined = jnp.concatenate(pieces, axis=1)
    for h in range(H):
        part[h] = joined[h * KB:(h + 1) * KB].astype(bf16)

    def gather(c, carry):
        at = pl.ds(pl.multiple_of(c * W, W), W)
        for s in range(NS):
            x = jnp.dot(hot[s], series_ref[s, :, at], preferred_element_type=f32)
            ep[s, :, at] = x.astype(bf16)
            x3 = x.reshape(EP, TR, W)
            total = jnp.sum(x3, axis=1)
            ssq = jnp.sum(x3 * x3, axis=1) - total * total * (1.0 / TR)
            inv[s, :, at] = shrink_factor * lax.rsqrt(jnp.maximum(ssq, 0.0) + series_floor)
        return carry

    after = chunks * C1 // 8
    pl.semaphore_wait(barrier, G + V - 2)

    def slab_copy(h, d, sender):
        return pltpu.make_async_remote_copy(
            src_ref=part.at[h], dst_ref=slots.at[h, sender],
            send_sem=slab_send.at[h, d], recv_sem=slab_recv.at[h, d],
            device_id=(subj, lax.rem(vox + d, V)),
            device_id_type=pl.DeviceIdType.MESH,
        )

    for h in range(H):
        for d in range(1, V):
            slab_copy(h, d, vox).start()

    out_row = iota((G * BR, 1), 0)
    within = lax.rem(out_row, BR)
    item = lax.rem(within, NR)
    source = (item // E1 * EP + lax.rem(item, E1)) * KB + within // NR * G + out_row // BR
    source = jnp.where(within < KH * NR, source, -1)
    perm[...] = jnp.where(source == iota((G * BR, KB * NE), 1), 1.0, 0.0).astype(bf16)

    full_row = iota((G * NE, 1), 0)
    epoch = lax.rem(full_row, EP)
    for i in range(KH):
        first = full_row // NE * NE + i * NR - starts[i] + lax.rem(full_row, NE) // EP * E1
        at = iota((G * NE, G * NE), 1) - first
        keep = jnp.where(at == epoch, 1.0, 0.0)
        rest = jnp.where(jnp.logical_and(at >= 0, at < E1), -1.0, 0.0)
        expand[i] = jnp.where(epoch < E1, keep, rest).astype(bf16)

    lax.fori_loop(0, after, gather, 0)

    same = iota((ROWS, ROWS), 0) // TR == iota((ROWS, ROWS), 1) // TR
    ones = jnp.where(same, 1.0, 0.0)
    pick_e = iota((EP, KB, ROWS), 2) // TR == iota((EP, KB, ROWS), 0)

    def slab_rows(h):
        slab = part[h].astype(f32)
        for d in range(1, V):
            slab_copy(h, d, lax.rem(vox - d + V, V)).wait_recv()
        for d in range(1, V):
            slab = slab + slots[h, lax.rem(vox + d, V)].astype(f32)
        rows = jnp.concatenate(
            [slab[:, s * ROWS:(s + 1) * ROWS] for s in range(NS)], axis=0
        )
        mean = jnp.dot(
            rows.astype(bf16), ones.astype(bf16), preferred_element_type=f32
        ) * (1.0 / TR)
        centred = rows - mean
        ssq = jnp.dot(
            centred * centred, ones,
            precision=lax.Precision.HIGHEST, preferred_element_type=f32,
        )
        std = centred / jnp.sqrt(ssq + series_floor)
        hi = std.astype(bf16).astype(f32)
        lo = std - hi
        for s in range(NS):
            for value, where in ((hi, a_hi), (lo, a_lo)):
                block = value[s * KB:(s + 1) * KB]
                spread = jnp.where(pick_e, block[None], 0.0).reshape(EP * KB, ROWS)
                where[h, s] = spread.astype(bf16)

    every = pl.ds(0, VL)

    def score_copy(h, to, sender, at):
        return pltpu.make_async_remote_copy(
            src_ref=send.at[h, to, :, at], dst_ref=recv.at[h, sender, :, at],
            send_sem=sc_send.at[h, to], recv_sem=sc_recv.at[h, sender],
            device_id=(to, vox), device_id_type=pl.DeviceIdType.MESH,
        )

    top = NE if KH > 1 else 0
    head_rows, tail_rows = pl.ds(0, top), pl.ds(top, BR - top)

    def last_copy(n, to, sender, at):
        rows = tail_rows if n < Q else head_rows
        return pltpu.make_async_remote_copy(
            src_ref=send.at[H - 1, to, rows, at], dst_ref=recv.at[H - 1, sender, rows, at],
            send_sem=last_send.at[n, to], recv_sem=last_recv.at[n, sender],
            device_id=(to, vox), device_id_type=pl.DeviceIdType.MESH,
        )

    def quarter(n):
        return pl.ds(n * QC, QC)

    last_parts = tuple((n, quarter(n)) for n in range(Q))
    if top:
        last_parts = ((Q, every),) + last_parts

    for h in range(H):
        slab_rows(h)

        def scores(c, carry, h=h):
            if h == 0 and after < chunks:
                @pl.when(c >= after)
                def _():
                    gather(c, 0)

            at = pl.ds(pl.multiple_of(c * W, W), W)
            parts = []
            for s in range(NS):
                x = ep[s, :, at]
                corr = jnp.dot(a_hi[h, s], x, preferred_element_type=f32)
                corr = corr + jnp.dot(a_lo[h, s], x, preferred_element_type=f32)
                r = corr.reshape(EP, KB, W) * inv[s, :, at][:, None, :]
                f = 0.5 * (jnp.log(1.0 + r) - jnp.log(1.0 - r))
                f = f - jnp.sum(f, axis=0, keepdims=True) * (1.0 / EP)
                var = jnp.sum(f * f, axis=0, keepdims=True) * (1.0 / EP)
                z = f * lax.rsqrt(var + spread_floor)
                parts.append(z.reshape(EP * KB, W).astype(bf16))
            z = jnp.concatenate(parts, axis=0)
            moved = jnp.dot(perm[...], z, preferred_element_type=f32)
            send[h, :, :, at] = moved.astype(bf16).reshape(G, BR, W)
            if h < H - 1:
                for to in cross + near:
                    score_copy(h, to, subj, at).start()
            recv[h, subj, :, at] = send[h, subj, :, at]
            return carry

        lax.fori_loop(0, chunks, scores, 0)

    for to in near + cross:
        for n, at in last_parts:
            last_copy(n, to, subj, at).start()

    def row_piece(r):
        return pl.ds(pl.multiple_of(r * RP, RP), RP)

    def part_copy(t, d):
        to = lax.rem(vox + d, V)
        return pltpu.make_async_remote_copy(
            src_ref=gram.at[t, row_piece(to // VR)], dst_ref=pieces_in.at[t, d - 1],
            send_sem=rs_send.at[t, d], recv_sem=rs_recv.at[t],
            device_id=(subj, to), device_id_type=pl.DeviceIdType.MESH,
        )

    def all_parts(t):
        return pltpu.make_async_remote_copy(
            src_ref=pieces_in.at[t], dst_ref=pieces_in.at[t],
            send_sem=rs_send.at[t, 0], recv_sem=rs_recv.at[t],
            device_id=(subj, lax.rem(vox + 1, V)), device_id_type=pl.DeviceIdType.MESH,
        )

    piece = vox // VR
    to_subj = piece // PG
    to_rows = lax.rem(piece, PG)

    def reduces(v):
        return lax.rem(v, VR) == 0

    def spot(t):
        p = t * G + subj
        return lax.rem(p + shift, V), p // V

    def final_copy(t):
        owner, local = spot(t)
        return pltpu.make_async_remote_copy(
            src_ref=summed.at[t], dst_ref=landed.at[local, to_rows],
            send_sem=fin_send.at[t], recv_sem=fin_recv.at[local, to_rows],
            device_id=(to_subj, owner), device_id_type=pl.DeviceIdType.MESH,
        )

    def away(t):
        owner, local = spot(t)
        return jnp.logical_or(to_subj != subj, owner != vox)

    def finish(t):
        @pl.when(reduces(vox))
        def _():
            all_parts(t).wait_recv()
            total = gram[t, row_piece(piece)]
            for d in range(1, V):
                total = total + pieces_in[t, d - 1]
            total = total * (1.0 / (VL * V))
            summed[t] = total

            @pl.when(away(t))
            def _():
                final_copy(t).start()

            @pl.when(jnp.logical_not(away(t)))
            def _():
                landed[spot(t)[1], to_rows] = total

    others = near + cross

    def add_gram(t, at, fresh):
        h, i = t // KH, t % KH
        rows = recv[h, :, starts[i]:starts[i] + NE, at].reshape(G * NE, -1)
        rows = jnp.dot(expand[i], rows, preferred_element_type=f32).astype(bf16)
        value = lax.dot_general(
            rows, rows, (((1,), (1,)), ((), ())), preferred_element_type=f32
        )
        gram[t] = value if fresh else gram[t] + value

    for t in range(T - 1):
        if t % KH == 0 and t < T - KH:
            for sender in others:
                score_copy(t // KH, sender, sender, every).wait_recv()
        if t == T - KH:
            for sender in others:
                last_copy(Q, sender, sender, every).wait_recv()
        for n in range(Q):
            add_gram(t, quarter(n), n == 0)
        for d in range(1, V):
            @pl.when(reduces(lax.rem(vox + d, V)))
            def _():
                part_copy(t, d).start()
        if t:
            finish(t - 1)

    for n in range(Q):
        for sender in others:
            last_copy(n, sender, sender, quarter(n)).wait_recv()
        add_gram(T - 1, quarter(n), n == 0)

    owner, local = spot(T - 1)

    def block(j):
        return pl.ds(j * NE, NE)

    def direct_copy(j):
        return pltpu.make_async_remote_copy(
            src_ref=gram.at[T - 1, block(j)], dst_ref=direct.at[vox],
            send_sem=dir_send.at[j], recv_sem=dir_recv.at[vox],
            device_id=(j, owner), device_id_type=pl.DeviceIdType.MESH,
        )

    def here(j):
        return jnp.logical_and(owner == vox, subj == j)

    for j in range(G):
        @pl.when(jnp.logical_not(here(j)))
        def _():
            direct_copy(j).start()

    if T > 1:
        finish(T - 2)

    for local in range(SL):
        p = local * V + lax.rem(vox - shift + 2 * V, V)
        handler = lax.rem(p, G)
        is_direct = p >= (T - 1) * G

        @pl.when(jnp.logical_not(is_direct))
        def _():
            for b in range(PG):
                source = (subj * PG + b) * VR

                @pl.when(jnp.logical_or(handler != subj, source != vox))
                def _():
                    pltpu.make_async_remote_copy(
                        src_ref=summed.at[0], dst_ref=landed.at[local, b],
                        send_sem=fin_send.at[0], recv_sem=fin_recv.at[local, b],
                        device_id=(subj, lax.rem(vox + 1, V)),
                        device_id_type=pl.DeviceIdType.MESH,
                    ).wait_recv()
                out_ref[local, b * RP:(b + 1) * RP] = landed[local, b]

        if (local + 1) * V > (T - 1) * G:
            @pl.when(is_direct)
            def _():
                @pl.when(handler == subj)
                def _():
                    direct[vox] = gram[T - 1, pl.ds(pl.multiple_of(subj * NE, NE), NE)]

                for v in range(V):
                    @pl.when(jnp.logical_or(handler != subj, v != vox))
                    def _():
                        pltpu.make_async_remote_copy(
                            src_ref=direct.at[v], dst_ref=direct.at[v],
                            send_sem=dir_send.at[0], recv_sem=dir_recv.at[v],
                            device_id=(subj, lax.rem(vox + 1, V)),
                            device_id_type=pl.DeviceIdType.MESH,
                        ).wait_recv()
                total = direct[0]
                for v in range(1, V):
                    total = total + direct[v]
                out_ref[local] = total * (1.0 / (VL * V))

    for h in range(H):
        for d in range(1, V):
            slab_copy(h, d, vox).wait_send()
        for to in others:
            if h < H - 1:
                score_copy(h, to, subj, every).wait_send()
            else:
                for n, at in last_parts:
                    last_copy(n, to, subj, at).wait_send()
    for t in range(T - 1):
        for d in range(1, V):
            @pl.when(reduces(lax.rem(vox + d, V)))
            def _():
                part_copy(t, d).wait_send()

        @pl.when(jnp.logical_and(reduces(vox), away(t)))
        def _():
            final_copy(t).wait_send()
    for j in range(G):
        @pl.when(jnp.logical_not(here(j)))
        def _():
            direct_copy(j).wait_send()


def body(series, offsets, selected):
    G = lax.axis_size("subj")
    V = lax.axis_size("vox")
    NS, RUN, VL = series.shape
    EP = offsets.shape[1]
    SEL = selected.shape[0]
    W = 256
    NE = NS * EP
    ROWS = EP * TR
    H = SEL // KB
    KH = KB // G
    SL = SEL // V
    R = pieces_of(G, V, NE)
    RP = G * NE // R
    BR = up8(KH * NS * (EP - 1))
    Q = 4
    vm = pltpu.VMEM
    dma = pltpu.SemaphoreType.DMA
    return pl.pallas_call(
        functools.partial(kernel, G, V, NS, EP, SEL, W),
        out_shape=jax.ShapeDtypeStruct((SL, NE, G * NE), f32),
        in_specs=[
            pl.BlockSpec(memory_space=pltpu.SMEM),
            pl.BlockSpec(memory_space=pltpu.SMEM),
            pl.BlockSpec(memory_space=pl.ANY),
        ],
        out_specs=pl.BlockSpec(memory_space=pltpu.VMEM),
        scratch_shapes=[
            vm((NS, RUN, VL), bf16),
            dma((NS,)),
            vm((NS, ROWS, VL), bf16),
            vm((NS, ROWS, RUN), bf16),
            vm((NS, EP, VL), f32),
            vm((H, KB, NS * ROWS), bf16),
            vm((H, V, KB, NS * ROWS), bf16),
            vm((H, NS, EP * KB, ROWS), bf16),
            vm((H, NS, EP * KB, ROWS), bf16),
            vm((G * BR, KB * NE), bf16),
            vm((H, G, BR, VL), bf16),
            vm((H, G, BR, VL), bf16),
            vm((KH, G * NE, G * NE), bf16),
            vm((H * KH, G * NE, G * NE), f32),
            vm((H * KH, V - 1, RP, G * NE), f32),
            vm((H * KH, RP, G * NE), f32),
            vm((SL, R // G, RP, G * NE), f32),
            vm((V, NE, G * NE), f32),
            dma((H, V)),
            dma((H, V)),
            dma((H, G)),
            dma((H, G)),
            dma((Q + 1, G)),
            dma((Q + 1, G)),
            dma((H * KH, V)),
            dma((H * KH,)),
            dma((H * KH,)),
            dma((SL, R // G)),
            dma((G,)),
            dma((V,)),
        ],
        compiler_params=pltpu.CompilerParams(
            collective_id=0, has_side_effects=True, vmem_limit_bytes=56 * 1024 * 1024
        ),
    )(offsets, selected, series)


def solution(mesh):
    placed = (P("subj", None, "vox"), P(), P())
    return jax.shard_map(
        body, mesh=mesh, in_specs=placed, out_specs=P("vox", "subj", None), check_vma=False
    )
```

```python
import functools

import jax
import jax.numpy as jnp
from jax import lax
from jax.experimental import pallas as pl
from jax.experimental.pallas import tpu as pltpu
from jax.sharding import PartitionSpec as P

TR = 16
KB = 8
C1 = 4
series_floor = 1.0
spread_floor = 0.05
shrink_factor = 0.9
f32 = jnp.float32
bf16 = jnp.bfloat16
MESH = pl.DeviceIdType.MESH


def iota(shape, dim):
    return lax.broadcasted_iota(jnp.int32, shape, dim)


def up8(n):
    return -(-n // 8) * 8


def pieces_of(G, V, NE):
    R = V
    while R > G and (V % R or R % G or (G * NE) % R or (G * NE // R) % 8):
        R -= 1
    return R


def column_groups(chunks):
    cuts = list(range(1, chunks, 2)) + [chunks]
    return tuple(zip(cuts[:-1], cuts[1:]))


def row_cuts(KI, NR, BR):
    return [0] + [min(up8((i + 1) * NR), BR) for i in range(KI)]


def flip(v, m):
    bit = 1
    while bit <= m:
        if m & bit:
            v = v + bit - 2 * bit * lax.rem(v // bit, 2)
        bit *= 2
    return v


def kernel(
    G, V, NS, EP, SEL, W,
    off_ref, sel_ref, series_hbm, out_ref,
    series_ref, load_sem, ep, inv, ep_far, inv_far, hot, part, slots, sums, sums_far,
    a_hi, a_lo, perm, send_far, send_near, send_emu, recv,
    gram, pair_in, pair_sum, pieces_in, last_in, summed, landed,
    slab_send, slab_recv, ep_send, ep_recv, sums_send, sums_recv,
    far_send, far_recv, last_send, last_recv, near_send, near_recv, emu_send, emu_recv,
    pair_send, pair_recv, rs_send, rs_recv, all_send, all_recv, fin_send, fin_recv,
):
    subj = lax.axis_index("subj")
    vox = lax.axis_index("vox")
    RUN = series_ref.shape[1]
    VL = series_ref.shape[2]
    ROWS = EP * TR
    SL = SEL // V
    NE = NS * EP
    chunks = VL // W
    R = pieces_of(G, V, NE)
    R2 = R // 2
    VR = V // R
    RP = G * NE // R
    PG = R // G
    HALF = G * NE // 2
    HG = G // 2
    HB = SEL // (2 * KB)
    KI = KB // HG
    T = HB * KI
    E1 = EP
    NR = NS * E1
    BR = recv.shape[2]
    starts = tuple(i * NR // 8 * 8 for i in range(KI))
    cuts = row_cuts(KI, NR, BR)
    groups = column_groups(chunks)
    shift = V // 2 + G // 2
    half = subj // HG
    core = lax.rem(subj, HG)
    far = [(1 - half) * HG + b for b in range(HG)]
    twin = (1 - half) * HG + core
    mates = [half * HG + lax.rem(core + d, HG) for d in range(1, HG)]

    barrier = pltpu.get_barrier_semaphore()
    for m in range(V - 1, 0, -1):
        pl.semaphore_signal(
            barrier, inc=1, device_id=(subj, flip(vox, m)), device_id_type=MESH,
        )
    for d in range(1, G):
        pl.semaphore_signal(
            barrier, inc=1, device_id=(lax.rem(subj + d, G), vox), device_id_type=MESH,
        )

    def load(s):
        return pltpu.make_async_copy(series_hbm.at[s], series_ref.at[s], load_sem.at[s])

    for s in range(NS):
        load(s).start()

    ids = jnp.zeros((SEL, 1), jnp.int32)
    which = iota((SEL, 1), 0)

    def chosen(kk, side):
        p = kk // HG * G + side * HG + kk % HG
        return sel_ref[(p + shift) % V * SL + p // V]

    for q in range(SEL):
        kk = q % (SEL // 2)
        swap = half == (0 if q < SEL // 2 else 1)
        ids = jnp.where(which == q, jnp.where(swap, chosen(kk, 1), chosen(kk, 0)), ids)
    picker = jnp.where(iota((SEL, VL), 1) + vox * VL == ids, 1.0, 0.0).astype(bf16)
    col = iota((TR, RUN), 1) - iota((TR, RUN), 0)
    pieces = []
    for s in range(NS):
        tiles = [
            jnp.where(col == off_ref[subj * NS + s, e], 1.0, 0.0) for e in range(EP)
        ]
        hot[s] = jnp.concatenate(tiles, axis=0).astype(bf16)
    for s in range(NS):
        load(s).wait()
        runs = lax.dot_general(
            picker, series_ref[s], (((1,), (1,)), ((), ())), preferred_element_type=f32
        )
        pieces.append(lax.dot_general(
            runs.astype(bf16), hot[s], (((1,), (1,)), ((), ())), preferred_element_type=f32
        ))
    joined = jnp.concatenate(pieces, axis=1)
    for h in range(2 * HB):
        part[h] = joined[h * KB:(h + 1) * KB].astype(bf16)

    def scale_of(x):
        x3 = x.reshape(EP, TR, W)
        total = jnp.sum(x3, axis=1)
        ssq = jnp.sum(x3 * x3, axis=1) - total * total * (1.0 / TR)
        return shrink_factor * lax.rsqrt(jnp.maximum(ssq, 0.0) + series_floor)

    def gather(c, carry):
        at = pl.ds(pl.multiple_of(c * W, W), W)
        for s in range(NS):
            x = jnp.dot(hot[s], series_ref[s, :, at], preferred_element_type=f32)
            ep[s, :, at] = x.astype(bf16)
            inv[s, :, at] = scale_of(x)
        return carry

    shared = pl.ds(0, W)
    gather(0, 0)
    after = max(chunks * C1 // 8, 1)
    pl.semaphore_wait(barrier, G + V - 2)

    def slab_copy(h, m):
        return pltpu.make_async_remote_copy(
            src_ref=part.at[h], dst_ref=slots.at[h, vox],
            send_sem=slab_send.at[h, m], recv_sem=slab_recv.at[h, m],
            device_id=(subj, flip(vox, m)), device_id_type=MESH,
        )

    def epoch_copy():
        return pltpu.make_async_remote_copy(
            src_ref=ep.at[:, :, shared], dst_ref=ep_far,
            send_sem=ep_send, recv_sem=ep_recv,
            device_id=(twin, vox), device_id_type=MESH,
        )

    def sums_copy(h):
        return pltpu.make_async_remote_copy(
            src_ref=sums.at[h], dst_ref=sums_far.at[h],
            send_sem=sums_send.at[h], recv_sem=sums_recv.at[h],
            device_id=(twin, vox), device_id_type=MESH,
        )

    for h in range(2 * HB):
        for m in range(V - 1, 0, -1):
            slab_copy(h, m).start()
        if h == 0:
            epoch_copy().start()

    out_row = iota((HG * BR, 1), 0)
    within = lax.rem(out_row, BR)
    item = lax.rem(within, NR)
    source = (item // E1 * EP + lax.rem(item, E1)) * KB + within // NR * HG + out_row // BR
    source = jnp.where(within < KI * NR, source, -1)
    perm[...] = jnp.where(source == iota((HG * BR, KB * NE), 1), 1.0, 0.0).astype(bf16)

    lax.fori_loop(1, after, gather, 0)

    same = iota((ROWS, ROWS), 0) // TR == iota((ROWS, ROWS), 1) // TR
    ones = jnp.where(same, 1.0, 0.0)
    pick_e = iota((EP, KB, ROWS), 2) // TR == iota((EP, KB, ROWS), 0)

    def standard_rows(h, slab):
        rows = jnp.concatenate(
            [slab[:, s * ROWS:(s + 1) * ROWS] for s in range(NS)], axis=0
        )
        mean = jnp.dot(
            rows.astype(bf16), ones.astype(bf16), preferred_element_type=f32
        ) * (1.0 / TR)
        centred = rows - mean
        ssq = jnp.dot(
            centred * centred, ones,
            precision=lax.Precision.HIGHEST, preferred_element_type=f32,
        )
        std = centred / jnp.sqrt(ssq + series_floor)
        hi = std.astype(bf16).astype(f32)
        lo = std - hi
        for s in range(NS):
            for value, where in ((hi, a_hi), (lo, a_lo)):
                block = value[s * KB:(s + 1) * KB]
                spread = jnp.where(pick_e, block[None], 0.0).reshape(EP * KB, ROWS)
                where[h, s] = spread.astype(bf16)

    def slab_sum(h):
        slab = part[h].astype(f32)
        for m in range(V - 1, 0, -1):
            slab_copy(h, m).wait_recv()
        for d in range(1, V):
            slab = slab + slots[h, lax.rem(vox + d, V)].astype(f32)
        return slab

    every = pl.ds(0, VL)

    def score(h, x_of, inv_of):
        parts = []
        for s in range(NS):
            x = x_of(s)
            corr = jnp.dot(a_hi[h, s], x, preferred_element_type=f32)
            corr = corr + jnp.dot(a_lo[h, s], x, preferred_element_type=f32)
            r = corr.reshape(EP, KB, W) * inv_of(s)[:, None, :]
            f = 0.5 * (jnp.log(1.0 + r) - jnp.log(1.0 - r))
            f = f - jnp.sum(f, axis=0, keepdims=True) * (1.0 / EP)
            var = jnp.sum(f * f, axis=0, keepdims=True) * (1.0 / EP)
            z = f * lax.rsqrt(var + spread_floor)
            parts.append(z.reshape(EP * KB, W).astype(bf16))
        z = jnp.concatenate(parts, axis=0)
        moved = jnp.dot(perm[...], z, preferred_element_type=f32)
        return moved.astype(bf16).reshape(HG, BR, W)

    def far_copy(h, b, sender, at):
        return pltpu.make_async_remote_copy(
            src_ref=send_far.at[h, b, :, at], dst_ref=recv.at[h, sender, :, at],
            send_sem=far_send.at[h, b], recv_sem=far_recv.at[h, lax.rem(sender, HG)],
            device_id=(far[b], vox), device_id_type=MESH,
        )

    P0 = len(groups) - 1

    def last_copy(n, b, sender, rows, at):
        rows = pl.ds(rows[0], rows[1] - rows[0])
        return pltpu.make_async_remote_copy(
            src_ref=send_far.at[HB - 1, b, rows, at],
            dst_ref=recv.at[HB - 1, sender, rows, at],
            send_sem=last_send.at[n, b], recv_sem=last_recv.at[n, lax.rem(sender, HG)],
            device_id=(far[b], vox), device_id_type=MESH,
        )

    def near_copy(h, d, sender, at):
        return pltpu.make_async_remote_copy(
            src_ref=send_near.at[h, lax.rem(mates[d - 1], HG), :, at],
            dst_ref=recv.at[h, sender, :, at],
            send_sem=near_send.at[h, d], recv_sem=near_recv.at[h, d],
            device_id=(mates[d - 1], vox), device_id_type=MESH,
        )

    def emu_copy(h, d, sender):
        return pltpu.make_async_remote_copy(
            src_ref=send_emu.at[h, lax.rem(mates[d - 1], HG)],
            dst_ref=recv.at[h, sender, :, shared],
            send_sem=emu_send.at[h, d], recv_sem=emu_recv.at[h, d],
            device_id=(mates[d - 1], vox), device_id_type=MESH,
        )

    beyond = pl.ds(W, VL - W)
    row_pieces = tuple(zip(cuts[:-1], cuts[1:]))
    last_plan = []
    for n, rows in enumerate(row_pieces):
        if rows[0] == rows[1]:
            continue
        if n < len(row_pieces) - 1:
            last_plan.append((n, rows, beyond))
        else:
            for g, (c0, c1) in enumerate(groups):
                last_plan.append((n + g, rows, pl.ds(c0 * W, (c1 - c0) * W)))

    for h in range(HB):
        slab = slab_sum(h)
        sums[h] = slab.astype(bf16)
        sums_copy(h).start()
        standard_rows(h, slab)

        def scores(c, carry, h=h):
            if h == 0 and after < chunks:
                @pl.when(c >= after)
                def _():
                    gather(c, 0)

            at = pl.ds(pl.multiple_of(c * W, W), W)
            send_far[h, :, :, at] = score(
                h, lambda s: ep[s, :, at], lambda s: inv[s, :, at]
            )
            for b in range(HG):
                if h < HB - 1:
                    far_copy(h, b, subj, at).start()
                elif cuts[1]:
                    last_copy(0, b, subj, row_pieces[0], at).start()
            return carry

        lax.fori_loop(1, chunks, scores, 0)
    for item_at in range(1, KI):
        closing = item_at == KI - 1
        for b in range(HG) if closing else range(HG - 1, -1, -1):
            for n, rows, at in last_plan:
                if rows == row_pieces[item_at]:
                    last_copy(n, b, subj, rows, at).start()

    for h in range(HB):
        standard_rows(HB + h, slab_sum(HB + h))

        def scores(c, carry, h=h):
            at = pl.ds(pl.multiple_of(c * W, W), W)
            send_near[h, :, :, at] = score(
                HB + h, lambda s: ep[s, :, at], lambda s: inv[s, :, at]
            )
            for d in range(1, HG):
                near_copy(h, d, subj, at).start()
            recv[h, subj, :, at] = send_near[h, core, :, at]
            return carry

        lax.fori_loop(0, chunks, scores, 0)

    epoch_copy().wait_recv()
    for s in range(NS):
        inv_far[s] = scale_of(ep_far[s].astype(f32))
    for h in range(HB):
        sums_copy(h).wait_recv()
        standard_rows(2 * HB + h, sums_far[h].astype(f32))
        send_emu[h] = score(2 * HB + h, lambda s: ep_far[s], lambda s: inv_far[s])
        for d in range(1, HG):
            emu_copy(h, d, twin).start()
        recv[h, twin, :, shared] = send_emu[h, core]

    def row_piece(r):
        return pl.ds(pl.multiple_of(r * RP, RP), RP)

    side, line = lax.rem(vox, 2), vox // 2
    pair = vox + 1 - 2 * side

    def pair_copy(t):
        rows = pl.ds(pl.multiple_of((1 - side) * HALF, HALF), HALF)
        return pltpu.make_async_remote_copy(
            src_ref=gram.at[t, rows], dst_ref=pair_in.at[t],
            send_sem=pair_send.at[t], recv_sem=pair_recv.at[t],
            device_id=(subj, pair), device_id_type=MESH,
        )

    def part_copy(t, m):
        to = flip(line, m)
        return pltpu.make_async_remote_copy(
            src_ref=pair_sum.at[t, row_piece(to // VR)], dst_ref=pieces_in.at[t, m - 1],
            send_sem=rs_send.at[t, m], recv_sem=rs_recv.at[t],
            device_id=(subj, to * 2 + side), device_id_type=MESH,
        )

    def all_parts(t):
        return pltpu.make_async_remote_copy(
            src_ref=pieces_in.at[t], dst_ref=pieces_in.at[t],
            send_sem=rs_send.at[t, 0], recv_sem=rs_recv.at[t],
            device_id=(subj, pair), device_id_type=MESH,
        )

    def piece_of(v):
        return lax.rem(v, 2) * R2 + v // 2 // VR

    def reduces(line):
        return lax.rem(line, VR) == 0

    TF = T - last_in.shape[0]

    def flat_copy(t, m):
        to = flip(vox, m)
        return pltpu.make_async_remote_copy(
            src_ref=gram.at[t, row_piece(piece_of(to))], dst_ref=last_in.at[t - TF, m - 1],
            send_sem=all_send.at[t - TF, m], recv_sem=all_recv.at[t - TF],
            device_id=(subj, to), device_id_type=MESH,
        )

    def flat_parts(t):
        return pltpu.make_async_remote_copy(
            src_ref=last_in.at[t - TF], dst_ref=last_in.at[t - TF],
            send_sem=all_send.at[t - TF, 0], recv_sem=all_recv.at[t - TF],
            device_id=(subj, pair), device_id_type=MESH,
        )

    piece = piece_of(vox)
    to_subj = piece // PG
    to_rows = lax.rem(piece, PG)

    def spot(t):
        p = t * G + subj
        return lax.rem(p + shift, V), p // V

    def final_copy(t):
        owner, local = spot(t)
        return pltpu.make_async_remote_copy(
            src_ref=summed.at[t], dst_ref=landed.at[local, to_rows],
            send_sem=fin_send.at[t], recv_sem=fin_recv.at[local, to_rows],
            device_id=(to_subj, owner), device_id_type=MESH,
        )

    def away(t):
        owner, local = spot(t)
        return jnp.logical_or(to_subj != subj, owner != vox)

    def middle(t):
        pair_copy(t).wait_recv()
        mine = pl.ds(pl.multiple_of(side * HALF, HALF), HALF)
        pair_sum[t] = gram[t, mine] + pair_in[t]
        for m in range(V // 2 - 1, 0, -1):
            @pl.when(reduces(flip(line, m)))
            def _():
                part_copy(t, m).start()

    def finish(t):
        @pl.when(reduces(line))
        def _():
            if t < TF:
                all_parts(t).wait_recv()
                total = pair_sum[t, row_piece(line // VR)]
                for d in range(V // 2 - 1):
                    total = total + pieces_in[t, d]
            else:
                flat_parts(t).wait_recv()
                total = gram[t, row_piece(piece)]
                for d in range(V - 1):
                    total = total + last_in[t - TF, d]
            total = total * (1.0 / (VL * V))
            summed[t] = total

            @pl.when(away(t))
            def _():
                final_copy(t).start()

            @pl.when(jnp.logical_not(away(t)))
            def _():
                landed[spot(t)[1], to_rows] = total

    def add_gram(t, c0, c1, fresh):
        h, i = t // KI, t % KI
        at = pl.ds(c0 * W, (c1 - c0) * W)
        rows = recv[h, :, starts[i]:starts[i] + NE, at].reshape(G * NE, -1)
        value = lax.dot_general(
            rows, rows, (((1,), (1,)), ((), ())), preferred_element_type=f32
        )
        gram[t] = value if fresh else gram[t] + value

    spans = tuple((c0 if g else 0, c1) for g, (c0, c1) in enumerate(groups))
    landed_rows = 0
    for t in range(T):
        h, i = t // KI, t % KI
        if i == 0:
            for d in range(1, HG):
                sender = half * HG + lax.rem(core - d + HG, HG)
                near_copy(h, d, sender, every).wait_recv()
                emu_copy(h, d, (1 - half) * HG + lax.rem(sender, HG)).wait_recv()
            landed_rows = 0
            if h < HB - 1:
                for b in range(HG):
                    far_copy(h, b, far[b], beyond).wait_recv()
                landed_rows = BR
        for g, (c0, c1) in enumerate(spans):
            for n, rows, at in last_plan:
                final = rows[1] == BR
                if final and (t < T - 1 or n != len(row_pieces) - 1 + g):
                    continue
                if h == HB - 1 and landed_rows < (i + 1) * NR and rows[0] == landed_rows:
                    for b in range(HG):
                        last_copy(n, b, far[b], rows, at).wait_recv()
                    if not final:
                        landed_rows = rows[1]
            add_gram(t, c0, c1, g == 0)
        if t < TF:
            pair_copy(t).start()
        else:
            for m in range(V - 1, 0, -1):
                @pl.when(reduces(flip(vox, m) // 2))
                def _():
                    flat_copy(t, m).start()
        if 0 < t <= TF:
            middle(t - 1)
        if 1 < t < T - 1:
            finish(t - 2)
    for t in range(max(T - 3, 0), T):
        finish(t)

    for local in range(SL):
        p = local * V + lax.rem(vox - shift + 2 * V, V)
        handler = lax.rem(p, G)
        for b in range(PG):
            owned = subj * PG + b
            source = lax.rem(owned, R2) * VR * 2 + owned // R2

            @pl.when(jnp.logical_or(handler != subj, source != vox))
            def _():
                pltpu.make_async_remote_copy(
                    src_ref=summed.at[0], dst_ref=landed.at[local, b],
                    send_sem=fin_send.at[0], recv_sem=fin_recv.at[local, b],
                    device_id=(subj, lax.rem(vox + 1, V)), device_id_type=MESH,
                ).wait_recv()
            out_ref[local, b * RP:(b + 1) * RP] = landed[local, b]

    for h in range(2 * HB):
        for m in range(1, V):
            slab_copy(h, m).wait_send()
    epoch_copy().wait_send()
    for h in range(HB):
        sums_copy(h).wait_send()
        for d in range(1, HG):
            near_copy(h, d, subj, every).wait_send()
            emu_copy(h, d, twin).wait_send()
        for b in range(HG):
            if h < HB - 1:
                far_copy(h, b, subj, beyond).wait_send()
            else:
                for n, rows, at in last_plan:
                    last_copy(n, b, subj, rows, at).wait_send()
    for t in range(T):
        if t >= TF:
            for m in range(1, V):
                @pl.when(reduces(flip(vox, m) // 2))
                def _():
                    flat_copy(t, m).wait_send()
        else:
            pair_copy(t).wait_send()
            for m in range(1, V // 2):
                @pl.when(reduces(flip(line, m)))
                def _():
                    part_copy(t, m).wait_send()

        @pl.when(jnp.logical_and(reduces(line), away(t)))
        def _():
            final_copy(t).wait_send()


def body(series, offsets, selected):
    G = lax.axis_size("subj")
    V = lax.axis_size("vox")
    NS, RUN, VL = series.shape
    EP = offsets.shape[1]
    SEL = selected.shape[0]
    W = 256
    NE = NS * EP
    ROWS = EP * TR
    HG = G // 2
    HB = SEL // (2 * KB)
    KI = KB // HG
    T = HB * KI
    NR = NS * EP
    BR = up8(KI * NR)
    SL = SEL // V
    R = pieces_of(G, V, NE)
    RP = G * NE // R
    chunks = VL // W
    plan = KI - 1 + len(column_groups(chunks))
    vm = pltpu.VMEM
    dma = pltpu.SemaphoreType.DMA
    return pl.pallas_call(
        functools.partial(kernel, G, V, NS, EP, SEL, W),
        out_shape=jax.ShapeDtypeStruct((SL, NE, G * NE), f32),
        in_specs=[
            pl.BlockSpec(memory_space=pltpu.SMEM),
            pl.BlockSpec(memory_space=pltpu.SMEM),
            pl.BlockSpec(memory_space=pl.ANY),
        ],
        out_specs=pl.BlockSpec(memory_space=pltpu.VMEM),
        scratch_shapes=[
            vm((NS, RUN, VL), bf16),
            dma((NS,)),
            vm((NS, ROWS, VL), bf16),
            vm((NS, EP, VL), f32),
            vm((NS, ROWS, W), bf16),
            vm((NS, EP, W), f32),
            vm((NS, ROWS, RUN), bf16),
            vm((2 * HB, KB, NS * ROWS), bf16),
            vm((2 * HB, V, KB, NS * ROWS), bf16),
            vm((HB, KB, NS * ROWS), bf16),
            vm((HB, KB, NS * ROWS), bf16),
            vm((3 * HB, NS, EP * KB, ROWS), bf16),
            vm((3 * HB, NS, EP * KB, ROWS), bf16),
            vm((HG * BR, KB * NE), bf16),
            vm((HB, HG, BR, VL), bf16),
            vm((HB, HG, BR, VL), bf16),
            vm((HB, HG, BR, W), bf16),
            vm((HB, G, BR, VL), bf16),
            vm((T, G * NE, G * NE), f32),
            vm((T, G * NE // 2, G * NE), f32),
            vm((T, G * NE // 2, G * NE), f32),
            vm((T, V // 2 - 1, RP, G * NE), f32),
            vm((min(3, T), V - 1, RP, G * NE), f32),
            vm((T, RP, G * NE), f32),
            vm((SL, R // G, RP, G * NE), f32),
            dma((2 * HB, V)),
            dma((2 * HB, V)),
            dma,
            dma,
            dma((HB,)),
            dma((HB,)),
            dma((HB, HG)),
            dma((HB, HG)),
            dma((plan, HG)),
            dma((plan, HG)),
            dma((HB, HG)),
            dma((HB, HG)),
            dma((HB, HG)),
            dma((HB, HG)),
            dma((T,)),
            dma((T,)),
            dma((T, V // 2)),
            dma((T,)),
            dma((min(3, T), V)),
            dma((min(3, T),)),
            dma((T,)),
            dma((SL, R // G)),
        ],
        compiler_params=pltpu.CompilerParams(
            collective_id=0, has_side_effects=True, vmem_limit_bytes=56 * 1024 * 1024
        ),
    )(offsets, selected, series)


def solution(mesh):
    placed = (P("subj", None, "vox"), P(), P())
    return jax.shard_map(
        body, mesh=mesh, in_specs=placed, out_specs=P("vox", "subj", None), check_vma=False
    )
```

```python
import functools

import jax
import jax.numpy as jnp
from jax import lax
from jax.experimental import pallas as pl
from jax.experimental.pallas import tpu as pltpu
from jax.sharding import PartitionSpec as P

TR = 16
KB = 8
C1 = 4
series_floor = 1.0
spread_floor = 0.05
shrink_factor = 0.9
f32 = jnp.float32
bf16 = jnp.bfloat16
MESH = pl.DeviceIdType.MESH


def iota(shape, dim):
    return lax.broadcasted_iota(jnp.int32, shape, dim)


def up8(n):
    return -(-n // 8) * 8


def pieces_of(G, V, NE):
    R = V
    while R > G and (V % R or R % G or (G * NE) % R or (G * NE // R) % 8):
        R -= 1
    return R


def column_groups(chunks):
    cuts = list(range(1, chunks, 2)) + [chunks]
    return tuple(zip(cuts[:-1], cuts[1:]))


def row_cuts(KI, NR, BR):
    return [0] + [min(up8((i + 1) * NR), BR) for i in range(KI)]


def flip(v, m):
    bit = 1
    while bit <= m:
        if m & bit:
            v = v + bit - 2 * bit * lax.rem(v // bit, 2)
        bit *= 2
    return v


def kernel(
    G, V, NS, EP, SEL, W,
    off_ref, sel_ref, series_hbm, out_ref,
    series_ref, load_sem, ep, inv, ep_far, inv_far, hot, part, slots, sums, sums_far,
    a_hi, a_lo, perm, send_far, send_near, send_emu, recv,
    gram, packed, pair_in, pair_sum, pieces_in, last_in, summed, landed,
    slab_send, slab_recv, ep_send, ep_recv, sums_send, sums_recv,
    far_send, far_recv, last_send, last_recv, near_send, near_recv, emu_send, emu_recv,
    pair_send, pair_recv, rs_send, rs_recv, all_send, all_recv, fin_send, fin_recv,
):
    subj = lax.axis_index("subj")
    vox = lax.axis_index("vox")
    RUN = series_ref.shape[1]
    VL = series_ref.shape[2]
    ROWS = EP * TR
    SL = SEL // V
    NE = NS * EP
    chunks = VL // W
    R = pieces_of(G, V, NE)
    R2 = R // 2
    VR = V // R
    RP = G * NE // R
    PG = R // G
    HALF = G * NE // 2
    HG = G // 2
    HB = SEL // (2 * KB)
    KI = KB // HG
    T = HB * KI
    E1 = EP
    NR = NS * E1
    BR = recv.shape[2]
    starts = tuple(i * NR // 8 * 8 for i in range(KI))
    cuts = row_cuts(KI, NR, BR)
    groups = column_groups(chunks)
    shift = V // 2 + G // 2
    half = subj // HG
    core = lax.rem(subj, HG)
    far = [(1 - half) * HG + b for b in range(HG)]
    twin = (1 - half) * HG + core
    mates = [half * HG + lax.rem(core + d, HG) for d in range(1, HG)]

    barrier = pltpu.get_barrier_semaphore()
    for m in range(V - 1, 0, -1):
        pl.semaphore_signal(
            barrier, inc=1, device_id=(subj, flip(vox, m)), device_id_type=MESH,
        )
    for d in range(1, G):
        pl.semaphore_signal(
            barrier, inc=1, device_id=(lax.rem(subj + d, G), vox), device_id_type=MESH,
        )

    def load(s):
        return pltpu.make_async_copy(series_hbm.at[s], series_ref.at[s], load_sem.at[s])

    for s in range(NS):
        load(s).start()

    ids = jnp.zeros((SEL, 1), jnp.int32)
    which = iota((SEL, 1), 0)

    def chosen(kk, side):
        p = kk // HG * G + side * HG + kk % HG
        return sel_ref[(p + shift) % V * SL + p // V]

    for q in range(SEL):
        kk = q % (SEL // 2)
        swap = half == (0 if q < SEL // 2 else 1)
        ids = jnp.where(which == q, jnp.where(swap, chosen(kk, 1), chosen(kk, 0)), ids)
    picker = jnp.where(iota((SEL, VL), 1) + vox * VL == ids, 1.0, 0.0).astype(bf16)
    col = iota((TR, RUN), 1) - iota((TR, RUN), 0)
    pieces = []
    for s in range(NS):
        tiles = [
            jnp.where(col == off_ref[subj * NS + s, e], 1.0, 0.0) for e in range(EP)
        ]
        hot[s] = jnp.concatenate(tiles, axis=0).astype(bf16)
    for s in range(NS):
        load(s).wait()
        runs = lax.dot_general(
            picker, series_ref[s], (((1,), (1,)), ((), ())), preferred_element_type=f32
        )
        pieces.append(lax.dot_general(
            runs.astype(bf16), hot[s], (((1,), (1,)), ((), ())), preferred_element_type=f32
        ))
    joined = jnp.concatenate(pieces, axis=1)
    for h in range(2 * HB):
        part[h] = joined[h * KB:(h + 1) * KB].astype(bf16)

    def scale_of(x):
        x3 = x.reshape(EP, TR, W)
        total = jnp.sum(x3, axis=1)
        ssq = jnp.sum(x3 * x3, axis=1) - total * total * (1.0 / TR)
        return shrink_factor * lax.rsqrt(jnp.maximum(ssq, 0.0) + series_floor)

    def gather(c, carry):
        at = pl.ds(pl.multiple_of(c * W, W), W)
        for s in range(NS):
            x = jnp.dot(hot[s], series_ref[s, :, at], preferred_element_type=f32)
            ep[s, :, at] = x.astype(bf16)
            inv[s, :, at] = scale_of(x)
        return carry

    shared = pl.ds(0, W)
    gather(0, 0)
    after = max(chunks * C1 // 8, 1)
    pl.semaphore_wait(barrier, G + V - 2)

    def slab_copy(h, m):
        return pltpu.make_async_remote_copy(
            src_ref=part.at[h], dst_ref=slots.at[h, vox],
            send_sem=slab_send.at[h, m], recv_sem=slab_recv.at[h, m],
            device_id=(subj, flip(vox, m)), device_id_type=MESH,
        )

    def epoch_copy():
        return pltpu.make_async_remote_copy(
            src_ref=ep.at[:, :, shared], dst_ref=ep_far,
            send_sem=ep_send, recv_sem=ep_recv,
            device_id=(twin, vox), device_id_type=MESH,
        )

    def sums_copy(h):
        return pltpu.make_async_remote_copy(
            src_ref=sums.at[h], dst_ref=sums_far.at[h],
            send_sem=sums_send.at[h], recv_sem=sums_recv.at[h],
            device_id=(twin, vox), device_id_type=MESH,
        )

    for h in range(2 * HB):
        for m in range(V - 1, 0, -1):
            slab_copy(h, m).start()
        if h == 0:
            epoch_copy().start()

    out_row = iota((HG * BR, 1), 0)
    within = lax.rem(out_row, BR)
    item = lax.rem(within, NR)
    source = (item // E1 * EP + lax.rem(item, E1)) * KB + within // NR * HG + out_row // BR
    source = jnp.where(within < KI * NR, source, -1)
    perm[...] = jnp.where(source == iota((HG * BR, KB * NE), 1), 1.0, 0.0).astype(bf16)

    lax.fori_loop(1, after, gather, 0)

    same = iota((ROWS, ROWS), 0) // TR == iota((ROWS, ROWS), 1) // TR
    ones = jnp.where(same, 1.0, 0.0)
    pick_e = iota((EP, KB, ROWS), 2) // TR == iota((EP, KB, ROWS), 0)

    def standard_rows(h, slab):
        rows = jnp.concatenate(
            [slab[:, s * ROWS:(s + 1) * ROWS] for s in range(NS)], axis=0
        )
        mean = jnp.dot(
            rows.astype(bf16), ones.astype(bf16), preferred_element_type=f32
        ) * (1.0 / TR)
        centred = rows - mean
        ssq = jnp.dot(
            centred * centred, ones,
            precision=lax.Precision.HIGHEST, preferred_element_type=f32,
        )
        std = centred / jnp.sqrt(ssq + series_floor)
        hi = std.astype(bf16).astype(f32)
        lo = std - hi
        for s in range(NS):
            for value, where in ((hi, a_hi), (lo, a_lo)):
                block = value[s * KB:(s + 1) * KB]
                spread = jnp.where(pick_e, block[None], 0.0).reshape(EP * KB, ROWS)
                where[h, s] = spread.astype(bf16)

    def slab_sum(h):
        slab = part[h].astype(f32)
        for m in range(V - 1, 0, -1):
            slab_copy(h, m).wait_recv()
        for d in range(1, V):
            slab = slab + slots[h, lax.rem(vox + d, V)].astype(f32)
        return slab

    every = pl.ds(0, VL)

    def score(h, x_of, inv_of):
        parts = []
        for s in range(NS):
            x = x_of(s)
            corr = jnp.dot(a_hi[h, s], x, preferred_element_type=f32)
            corr = corr + jnp.dot(a_lo[h, s], x, preferred_element_type=f32)
            r = corr.reshape(EP, KB, W) * inv_of(s)[:, None, :]
            f = 0.5 * (jnp.log(1.0 + r) - jnp.log(1.0 - r))
            f = f - jnp.sum(f, axis=0, keepdims=True) * (1.0 / EP)
            var = jnp.sum(f * f, axis=0, keepdims=True) * (1.0 / EP)
            z = f * lax.rsqrt(var + spread_floor)
            parts.append(z.reshape(EP * KB, W).astype(bf16))
        z = jnp.concatenate(parts, axis=0)
        moved = jnp.dot(perm[...], z, preferred_element_type=f32)
        return moved.astype(bf16).reshape(HG, BR, W)

    def far_copy(h, b, sender, at):
        return pltpu.make_async_remote_copy(
            src_ref=send_far.at[h, b, :, at], dst_ref=recv.at[h, sender, :, at],
            send_sem=far_send.at[h, b], recv_sem=far_recv.at[h, lax.rem(sender, HG)],
            device_id=(far[b], vox), device_id_type=MESH,
        )

    P0 = len(groups) - 1

    def last_copy(n, b, sender, rows, at):
        rows = pl.ds(rows[0], rows[1] - rows[0])
        return pltpu.make_async_remote_copy(
            src_ref=send_far.at[HB - 1, b, rows, at],
            dst_ref=recv.at[HB - 1, sender, rows, at],
            send_sem=last_send.at[n, b], recv_sem=last_recv.at[n, lax.rem(sender, HG)],
            device_id=(far[b], vox), device_id_type=MESH,
        )

    def near_copy(h, d, sender, at):
        return pltpu.make_async_remote_copy(
            src_ref=send_near.at[h, lax.rem(mates[d - 1], HG), :, at],
            dst_ref=recv.at[h, sender, :, at],
            send_sem=near_send.at[h, d], recv_sem=near_recv.at[h, d],
            device_id=(mates[d - 1], vox), device_id_type=MESH,
        )

    def emu_copy(h, d, sender):
        return pltpu.make_async_remote_copy(
            src_ref=send_emu.at[h, lax.rem(mates[d - 1], HG)],
            dst_ref=recv.at[h, sender, :, shared],
            send_sem=emu_send.at[h, d], recv_sem=emu_recv.at[h, d],
            device_id=(mates[d - 1], vox), device_id_type=MESH,
        )

    beyond = pl.ds(W, VL - W)
    row_pieces = tuple(zip(cuts[:-1], cuts[1:]))
    last_plan = []
    for n, rows in enumerate(row_pieces):
        if rows[0] == rows[1]:
            continue
        if n < len(row_pieces) - 1:
            last_plan.append((n, rows, beyond))
        else:
            for g, (c0, c1) in enumerate(groups):
                last_plan.append((n + g, rows, pl.ds(c0 * W, (c1 - c0) * W)))

    for h in range(HB):
        slab = slab_sum(h)
        sums[h] = slab.astype(bf16)
        sums_copy(h).start()
        standard_rows(h, slab)

        def scores(c, carry, h=h):
            if h == 0 and after < chunks:
                @pl.when(c >= after)
                def _():
                    gather(c, 0)

            at = pl.ds(pl.multiple_of(c * W, W), W)
            send_far[h, :, :, at] = score(
                h, lambda s: ep[s, :, at], lambda s: inv[s, :, at]
            )
            for b in range(HG):
                if h < HB - 1:
                    far_copy(h, b, subj, at).start()
                elif cuts[1]:
                    last_copy(0, b, subj, row_pieces[0], at).start()
            return carry

        lax.fori_loop(1, chunks, scores, 0)
    for item_at in range(1, KI):
        closing = item_at == KI - 1
        for b in range(HG) if closing else range(HG - 1, -1, -1):
            for n, rows, at in last_plan:
                if rows == row_pieces[item_at]:
                    last_copy(n, b, subj, rows, at).start()

    for h in range(HB):
        standard_rows(HB + h, slab_sum(HB + h))

        def scores(c, carry, h=h):
            at = pl.ds(pl.multiple_of(c * W, W), W)
            send_near[h, :, :, at] = score(
                HB + h, lambda s: ep[s, :, at], lambda s: inv[s, :, at]
            )
            for d in range(1, HG):
                near_copy(h, d, subj, at).start()
            recv[h, subj, :, at] = send_near[h, core, :, at]
            return carry

        lax.fori_loop(0, chunks, scores, 0)

    epoch_copy().wait_recv()
    for s in range(NS):
        inv_far[s] = scale_of(ep_far[s].astype(f32))
    for h in range(HB):
        sums_copy(h).wait_recv()
        standard_rows(2 * HB + h, sums_far[h].astype(f32))
        send_emu[h] = score(2 * HB + h, lambda s: ep_far[s], lambda s: inv_far[s])
        for d in range(1, HG):
            emu_copy(h, d, twin).start()
        recv[h, twin, :, shared] = send_emu[h, core]

    def row_piece(r):
        return pl.ds(pl.multiple_of(r * RP, RP), RP)

    side, line = lax.rem(vox, 2), vox // 2
    pair = vox + 1 - 2 * side

    def pair_copy(t):
        rows = pl.ds(pl.multiple_of((1 - side) * HALF, HALF), HALF)
        return pltpu.make_async_remote_copy(
            src_ref=gram.at[t, rows], dst_ref=pair_in.at[t],
            send_sem=pair_send.at[t], recv_sem=pair_recv.at[t],
            device_id=(subj, pair), device_id_type=MESH,
        )

    def part_copy(t, m):
        to = flip(line, m)
        return pltpu.make_async_remote_copy(
            src_ref=pair_sum.at[t, row_piece(to // VR)], dst_ref=pieces_in.at[t, m - 1],
            send_sem=rs_send.at[t, m], recv_sem=rs_recv.at[t],
            device_id=(subj, to * 2 + side), device_id_type=MESH,
        )

    def all_parts(t):
        return pltpu.make_async_remote_copy(
            src_ref=pieces_in.at[t], dst_ref=pieces_in.at[t],
            send_sem=rs_send.at[t, 0], recv_sem=rs_recv.at[t],
            device_id=(subj, pair), device_id_type=MESH,
        )

    def piece_of(v):
        return lax.rem(v, 2) * R2 + v // 2 // VR

    def reduces(line):
        return lax.rem(line, VR) == 0

    TF = T - last_in.shape[0]

    def flat_copy(t, m):
        to = flip(vox, m)
        return pltpu.make_async_remote_copy(
            src_ref=packed.at[t - TF, piece_of(to)], dst_ref=last_in.at[t - TF, m - 1],
            send_sem=all_send.at[t - TF, m], recv_sem=all_recv.at[t - TF],
            device_id=(subj, to), device_id_type=MESH,
        )

    LEFT = G * NE // 128 * 128
    REST = G * NE - LEFT
    TALL = packed.shape[2] - RP

    def pack(t):
        for p in range(R):
            rows = gram[t, p * RP:(p + 1) * RP]
            packed[t - TF, p, :RP] = rows[:, :LEFT]
            packed[t - TF, p, RP:, :REST] = rows[:TALL, LEFT:]
            packed[t - TF, p, RP:2 * RP - TALL, REST:2 * REST] = rows[TALL:, LEFT:]

    def flat_parts(t):
        return pltpu.make_async_remote_copy(
            src_ref=last_in.at[t - TF], dst_ref=last_in.at[t - TF],
            send_sem=all_send.at[t - TF, 0], recv_sem=all_recv.at[t - TF],
            device_id=(subj, pair), device_id_type=MESH,
        )

    piece = piece_of(vox)
    to_subj = piece // PG
    to_rows = lax.rem(piece, PG)

    def spot(t):
        p = t * G + subj
        return lax.rem(p + shift, V), p // V

    def final_copy(t):
        owner, local = spot(t)
        return pltpu.make_async_remote_copy(
            src_ref=summed.at[t], dst_ref=landed.at[local, to_rows],
            send_sem=fin_send.at[t], recv_sem=fin_recv.at[local, to_rows],
            device_id=(to_subj, owner), device_id_type=MESH,
        )

    def away(t):
        owner, local = spot(t)
        return jnp.logical_or(to_subj != subj, owner != vox)

    def middle(t):
        pair_copy(t).wait_recv()
        mine = pl.ds(pl.multiple_of(side * HALF, HALF), HALF)
        pair_sum[t] = gram[t, mine] + pair_in[t]
        for m in range(V // 2 - 1, 0, -1):
            @pl.when(reduces(flip(line, m)))
            def _():
                part_copy(t, m).start()

    def finish(t):
        @pl.when(reduces(line))
        def _():
            if t < TF:
                all_parts(t).wait_recv()
                total = pair_sum[t, row_piece(line // VR)]
                for d in range(V // 2 - 1):
                    total = total + pieces_in[t, d]
            else:
                flat_parts(t).wait_recv()
                total = packed[t - TF, piece]
                for d in range(V - 1):
                    total = total + last_in[t - TF, d]
            total = total * (1.0 / (VL * V))
            if t >= TF:
                rest = jnp.concatenate(
                    [total[RP:, :REST], total[RP:2 * RP - TALL, REST:2 * REST]], axis=0
                )
                total = jnp.concatenate([total[:RP], rest], axis=1)
            summed[t] = total

            @pl.when(away(t))
            def _():
                final_copy(t).start()

            @pl.when(jnp.logical_not(away(t)))
            def _():
                landed[spot(t)[1], to_rows] = total

    def add_gram(t, c0, c1, fresh):
        h, i = t // KI, t % KI
        at = pl.ds(c0 * W, (c1 - c0) * W)
        rows = recv[h, :, starts[i]:starts[i] + NE, at].reshape(G * NE, -1)
        value = lax.dot_general(
            rows, rows, (((1,), (1,)), ((), ())), preferred_element_type=f32
        )
        gram[t] = value if fresh else gram[t] + value

    spans = tuple((c0 if g else 0, c1) for g, (c0, c1) in enumerate(groups))
    landed_rows = 0
    for t in range(T):
        h, i = t // KI, t % KI
        if i == 0:
            for d in range(1, HG):
                sender = half * HG + lax.rem(core - d + HG, HG)
                near_copy(h, d, sender, every).wait_recv()
                emu_copy(h, d, (1 - half) * HG + lax.rem(sender, HG)).wait_recv()
            landed_rows = 0
            if h < HB - 1:
                for b in range(HG):
                    far_copy(h, b, far[b], beyond).wait_recv()
                landed_rows = BR
        for g, (c0, c1) in enumerate(spans):
            for n, rows, at in last_plan:
                final = rows[1] == BR
                if final and (t < T - 1 or n != len(row_pieces) - 1 + g):
                    continue
                if h == HB - 1 and landed_rows < (i + 1) * NR and rows[0] == landed_rows:
                    for b in range(HG):
                        last_copy(n, b, far[b], rows, at).wait_recv()
                    if not final:
                        landed_rows = rows[1]
            add_gram(t, c0, c1, g == 0)
        if t < TF:
            pair_copy(t).start()
        else:
            pack(t)
            for m in range(V - 1, 0, -1):
                @pl.when(reduces(flip(vox, m) // 2))
                def _():
                    flat_copy(t, m).start()
        if 0 < t <= TF:
            middle(t - 1)
        if 1 < t < T - 1:
            finish(t - 2)
    for t in range(max(T - 3, 0), T):
        finish(t)

    for local in range(SL):
        p = local * V + lax.rem(vox - shift + 2 * V, V)
        handler = lax.rem(p, G)
        for b in range(PG):
            owned = subj * PG + b
            source = lax.rem(owned, R2) * VR * 2 + owned // R2

            @pl.when(jnp.logical_or(handler != subj, source != vox))
            def _():
                pltpu.make_async_remote_copy(
                    src_ref=summed.at[0], dst_ref=landed.at[local, b],
                    send_sem=fin_send.at[0], recv_sem=fin_recv.at[local, b],
                    device_id=(subj, lax.rem(vox + 1, V)), device_id_type=MESH,
                ).wait_recv()
            out_ref[local, b * RP:(b + 1) * RP] = landed[local, b]

    for h in range(2 * HB):
        for m in range(1, V):
            slab_copy(h, m).wait_send()
    epoch_copy().wait_send()
    for h in range(HB):
        sums_copy(h).wait_send()
        for d in range(1, HG):
            near_copy(h, d, subj, every).wait_send()
            emu_copy(h, d, twin).wait_send()
        for b in range(HG):
            if h < HB - 1:
                far_copy(h, b, subj, beyond).wait_send()
            else:
                for n, rows, at in last_plan:
                    last_copy(n, b, subj, rows, at).wait_send()
    for t in range(T):
        if t >= TF:
            for m in range(1, V):
                @pl.when(reduces(flip(vox, m) // 2))
                def _():
                    flat_copy(t, m).wait_send()
        else:
            pair_copy(t).wait_send()
            for m in range(1, V // 2):
                @pl.when(reduces(flip(line, m)))
                def _():
                    part_copy(t, m).wait_send()

        @pl.when(jnp.logical_and(reduces(line), away(t)))
        def _():
            final_copy(t).wait_send()


def body(series, offsets, selected):
    G = lax.axis_size("subj")
    V = lax.axis_size("vox")
    NS, RUN, VL = series.shape
    EP = offsets.shape[1]
    SEL = selected.shape[0]
    W = 256
    NE = NS * EP
    ROWS = EP * TR
    HG = G // 2
    HB = SEL // (2 * KB)
    KI = KB // HG
    T = HB * KI
    NR = NS * EP
    BR = up8(KI * NR)
    SL = SEL // V
    R = pieces_of(G, V, NE)
    RP = G * NE // R
    chunks = VL // W
    plan = KI - 1 + len(column_groups(chunks))
    vm = pltpu.VMEM
    dma = pltpu.SemaphoreType.DMA
    return pl.pallas_call(
        functools.partial(kernel, G, V, NS, EP, SEL, W),
        out_shape=jax.ShapeDtypeStruct((SL, NE, G * NE), f32),
        in_specs=[
            pl.BlockSpec(memory_space=pltpu.SMEM),
            pl.BlockSpec(memory_space=pltpu.SMEM),
            pl.BlockSpec(memory_space=pl.ANY),
        ],
        out_specs=pl.BlockSpec(memory_space=pltpu.VMEM),
        scratch_shapes=[
            vm((NS, RUN, VL), bf16),
            dma((NS,)),
            vm((NS, ROWS, VL), bf16),
            vm((NS, EP, VL), f32),
            vm((NS, ROWS, W), bf16),
            vm((NS, EP, W), f32),
            vm((NS, ROWS, RUN), bf16),
            vm((2 * HB, KB, NS * ROWS), bf16),
            vm((2 * HB, V, KB, NS * ROWS), bf16),
            vm((HB, KB, NS * ROWS), bf16),
            vm((HB, KB, NS * ROWS), bf16),
            vm((3 * HB, NS, EP * KB, ROWS), bf16),
            vm((3 * HB, NS, EP * KB, ROWS), bf16),
            vm((HG * BR, KB * NE), bf16),
            vm((HB, HG, BR, VL), bf16),
            vm((HB, HG, BR, VL), bf16),
            vm((HB, HG, BR, W), bf16),
            vm((HB, G, BR, VL), bf16),
            vm((T, G * NE, G * NE), f32),
            vm((min(2, T), R, RP + up8(-(-RP // 2)), G * NE // 128 * 128), f32),
            vm((T, G * NE // 2, G * NE), f32),
            vm((T, G * NE // 2, G * NE), f32),
            vm((T, V // 2 - 1, RP, G * NE), f32),
            vm((min(2, T), V - 1, RP + up8(-(-RP // 2)), G * NE // 128 * 128), f32),
            vm((T, RP, G * NE), f32),
            vm((SL, R // G, RP, G * NE), f32),
            dma((2 * HB, V)),
            dma((2 * HB, V)),
            dma,
            dma,
            dma((HB,)),
            dma((HB,)),
            dma((HB, HG)),
            dma((HB, HG)),
            dma((plan, HG)),
            dma((plan, HG)),
            dma((HB, HG)),
            dma((HB, HG)),
            dma((HB, HG)),
            dma((HB, HG)),
            dma((T,)),
            dma((T,)),
            dma((T, V // 2)),
            dma((T,)),
            dma((min(2, T), V)),
            dma((min(2, T),)),
            dma((T,)),
            dma((SL, R // G)),
        ],
        compiler_params=pltpu.CompilerParams(
            collective_id=0, has_side_effects=True, vmem_limit_bytes=56 * 1024 * 1024
        ),
    )(offsets, selected, series)


def solution(mesh):
    placed = (P("subj", None, "vox"), P(), P())
    return jax.shard_map(
        body, mesh=mesh, in_specs=placed, out_specs=P("vox", "subj", None), check_vma=False
    )
```
